32 devices in a mesh: pp: 4 (over x, core), tp: 4 (over z), dp: 2 (over y).
Axes of the slice: x: 2, y: 2, z: 4, core: 2. Of those that a mesh axis runs over, the one named last changes fastest.
Arguments:
- act_in: bfloat16 [4, 2, 128, 4096], P('pp', 'dp', 'tp'), may hold values from -6 to 6
- stash_in: bfloat16 [4, 2, 128, 4096], P('pp', 'dp', 'tp'), may hold values from -6 to 6
- grad_in: bfloat16 [4, 2, 128, 4096], P('pp', 'dp', 'tp'), may hold values from -6 to 6
- doc_ids: int32 [4, 2, 2, 128], P('pp', 'dp'), may hold values from 0 to 15, never falling along the last dimension, each value on 1 to 64 neighbouring positions
- query_weight: bfloat16 [4, 4096, 4096], P('pp', None, 'tp'), as said below
- key_weight: bfloat16 [4, 4096, 1024], P('pp', None, 'tp'), as said below
- value_weight: bfloat16 [4, 4096, 1024], P('pp', None, 'tp'), as said below
- out_weight: bfloat16 [4, 4096, 4096], P('pp', None, 'tp'), may hold values from -0.09375 to 0.09375
Outputs:
- act_out: bfloat16 [4, 2, 128, 4096], P('pp', 'dp', 'tp')
- grad_out: bfloat16 [4, 2, 128, 4096], P('pp', 'dp', 'tp')
- grad_query: float32 [4, 4096, 4096], P('pp', 'dp', 'tp')
- grad_key: float32 [4, 4096, 1024], P('pp', 'dp', 'tp')
- grad_value: float32 [4, 4096, 1024], P('pp', 'dp', 'tp')
The draws below stay inside these ranges and needn't reach their ends.
Inputs may be any that keep to these rules, and one draw needn't show every extreme that they name: `doc_ids`: along each row of 128 positions the document numbers never fall. `query_weight`: entries of mean zero. `key_weight`: for each of the 8 key heads, its 1 stored copies (consecutive blocks of 128 columns) are equal; entries of mean zero. `value_weight`: for each of the 8 value heads, its 1 stored copies (consecutive blocks of 128 columns) are equal.
All inputs are finite; a program needn't handle non-finite values.
Results may differ from the reference program's by a relative error of at most 0.033.
Values may be sent and summed in bfloat16 or wider, within the bound.
A program may use at most 128 MiB of HBM per device.

```python
import math
import jax
import jax.numpy as jnp
import numpy as np
from jax import lax

D = 4096
HEADS = 32
KV = 8
HEAD = 128
SEQ = 128
SPREAD = 1
N_PP = 4
N_TP = 4
N_DP = 2


def shared_heads(key, salt):
    base = jax.random.normal(jax.random.fold_in(key, salt), (N_PP, D, KV, 1, HEAD), jnp.float32)
    base = jnp.clip(base, -5.0, 5.0) / math.sqrt(D)
    return jnp.broadcast_to(base, (N_PP, D, KV, SPREAD, HEAD)).reshape(N_PP, D, KV * SPREAD, HEAD)


def draw_key_weight(key, part):
    return shared_heads(key, 11).reshape(N_PP, D, KV * SPREAD * HEAD).astype(jnp.bfloat16)


def draw_value_weight(key, part):
    return shared_heads(key, 13).reshape(N_PP, D, KV * SPREAD * HEAD).astype(jnp.bfloat16)


def draw_query_weight(key, part):
    fresh = jax.random.normal(jax.random.fold_in(key, 12), (N_PP, D, HEADS * HEAD), jnp.float32)
    fresh = jnp.clip(fresh, -5.0, 5.0) / math.sqrt(D)
    return fresh.astype(jnp.bfloat16)


def block_levels(key, dims, cuts, least, top_value):
    loudness = 1.0
    for axis_at, shards_of in cuts:
        heights = jax.random.uniform(jax.random.fold_in(jax.random.fold_in(key, 6), axis_at), (shards_of,), jnp.float32, least / len(cuts), top_value / len(cuts))
        loudness = loudness * jnp.repeat(jnp.exp(heights), dims[axis_at] // shards_of).reshape((-1,) + (1,) * (len(dims) - 1 - axis_at))
    return loudness


def profile(count, total, reach, skew):
    weights = [(1 << 20) // math.isqrt(grade ** skew) + 1 for grade in range(2, count + 1)]
    spare, given = total - reach - (count - 1), [1] * (count - 1)
    while spare > 0:
        movable = [i for i in range(count - 1) if given[i] < reach]
        whole, left = sum([weights[i] for i in movable]), spare
        for i in movable:
            addition = min(reach - given[i], max(1, left * weights[i] // whole), spare)
            given[i] = given[i] + addition
            spare = spare - addition
    return np.array([reach] + given)


def ragged_sizes(own_key, count, total, limit, slope):
    if count == 2:
        one = jax.random.randint(own_key, (), max(1, total - limit), min(limit, total - 1) + 1)
        return jnp.stack([one, total - one])
    lengths = jnp.asarray(profile(count, total, limit, slope), jnp.int32)
    twos = (count - 1) // 2
    giver, sink = lengths[1:1 + 2 * twos:2], lengths[2:2 + 2 * twos:2]
    room = jnp.minimum(giver - 1, limit - sink)
    passed = jax.random.randint(jax.random.fold_in(own_key, 1), (twos,), 0, 1 << 20) % (room + 1)
    lengths = lengths.at[1:1 + 2 * twos:2].set(giver - passed).at[2:2 + 2 * twos:2].set(sink + passed)
    return lengths[jax.random.permutation(jax.random.fold_in(own_key, 2), count)]


def noise(key, shape, deviation, limit, split=(), held_as=jnp.bfloat16):
    result = deviation * jax.random.normal(key, shape, jnp.float32)
    if split:
        result = result * block_levels(key, shape, split, -0.22, 0.18)
    return jnp.clip(result, -limit, limit).astype(held_as)


def setup_inputs(seed: int = 0) -> dict:
    streams_of = jax.random.split(jax.random.key(seed), 9)
    return {
        "act_in": noise(streams_of[0], (N_PP, N_DP, SEQ, D), 1.0, 6.0, ((0, 4), (1, 2), (2, 4))),
        "stash_in": noise(streams_of[1], (N_PP, N_DP, SEQ, D), 1.0, 6.0, ((0, 4), (1, 2), (2, 4))),
        "grad_in": noise(streams_of[2], (N_PP, N_DP, SEQ, D), 1.0, 6.0, ((0, 4), (1, 2), (2, 4))),
        "doc_ids": jax.vmap(lambda own: jnp.searchsorted(jnp.cumsum(ragged_sizes(own, SEQ // 8, SEQ, SEQ // 2, 2)), jnp.arange(SEQ), side="right"))(jax.random.split(streams_of[3], N_PP * N_DP * 2)).reshape((N_PP, N_DP, 2, SEQ)).astype(jnp.int32),
        "query_weight": draw_query_weight(jax.random.fold_in(streams_of[8], 71), 0),
        "key_weight": draw_key_weight(jax.random.fold_in(streams_of[8], 71), 0),
        "value_weight": draw_value_weight(jax.random.fold_in(streams_of[8], 71), 0),
        "out_weight": noise(streams_of[7], (N_PP, D, HEADS * HEAD), (HEADS * HEAD) ** -0.5, 0.09375, ((0, 4), (2, 4))),
    }


epsilon = 1e-05

def norm_rows(token_rows):
    widened = token_rows.astype(jnp.float32)
    inverse = lax.rsqrt(lax.optimization_barrier(jnp.mean(widened * widened, axis=-1, keepdims=True)) + epsilon)
    return ((widened * inverse).astype(jnp.bfloat16), inverse)

def allowed(documents):
    length = documents.shape[0]
    position = jnp.arange(length, dtype=jnp.int32)
    return (position[None, :] <= position[:, None]) & (documents[:, None] == documents[None, :])

def project(normed, weight):
    return jnp.dot(normed, weight, preferred_element_type=jnp.float32).astype(jnp.bfloat16)

def contract_first(left_side, right_side):
    return lax.dot_general(left_side, right_side, (((0,), (0,)), ((), ())), preferred_element_type=jnp.float32)

def split_heads(queries, keys, values):
    length = queries.shape[0]
    key_count = KV * SPREAD
    group_size = HEADS // key_count
    query_heads = queries.astype(jnp.float32).reshape(length, key_count, group_size, HEAD)
    key_heads = keys.astype(jnp.float32).reshape(length, key_count, HEAD)
    value_heads = values.astype(jnp.float32).reshape(length, key_count, HEAD)
    return (query_heads, key_heads, value_heads)

def attend(queries, keys, values, allowed_pairs):
    length = queries.shape[0]
    query_heads, key_heads, value_heads = split_heads(queries, keys, values)
    scores = jnp.einsum('ihgd,jhd->hgij', query_heads, key_heads) * (1.0 / math.sqrt(HEAD))
    scores = jnp.where(allowed_pairs, scores, -jnp.inf)
    row_max = lax.optimization_barrier(jnp.max(scores, axis=-1, keepdims=True))
    weights = jnp.exp(scores - row_max)
    probs = (weights / lax.optimization_barrier(jnp.sum(weights, axis=-1, keepdims=True))).astype(jnp.bfloat16)
    mixed = jnp.einsum('hgij,jhd->ihgd', probs.astype(jnp.float32), value_heads)
    return (probs, mixed.astype(jnp.bfloat16).reshape(length, HEADS * HEAD))

def attend_back(dmixed, queries, keys, values, probs):
    length = queries.shape[0]
    query_heads, key_heads, value_heads = split_heads(queries, keys, values)
    dmixed_heads = dmixed.astype(jnp.float32).reshape(query_heads.shape)
    dprobs = jnp.einsum('ihgd,jhd->hgij', dmixed_heads, value_heads)
    weights = probs.astype(jnp.float32)
    inner = lax.optimization_barrier(jnp.sum(weights * dprobs, axis=-1, keepdims=True))
    dscores = (weights * (dprobs - inner) * (1.0 / math.sqrt(HEAD))).astype(jnp.bfloat16)
    dqueries = jnp.einsum('hgij,jhd->ihgd', dscores.astype(jnp.float32), key_heads)
    dkeys = jnp.einsum('hgij,ihgd->jhd', dscores.astype(jnp.float32), query_heads)
    dvalues = jnp.einsum('hgij,ihgd->jhd', weights, dmixed_heads)
    return (dqueries.astype(jnp.bfloat16).reshape(length, HEADS * HEAD), dkeys.reshape(length, KV * SPREAD * HEAD), dvalues.reshape(length, KV * SPREAD * HEAD))

def rounded(product):
    return lax.optimization_barrier(product.astype(jnp.bfloat16)).astype(jnp.float32)

def group_sum(pairs):
    total = None
    for left_side, weight in pairs:
        length = left_side.shape[0]
        width = left_side.shape[1] // N_TP
        term = jnp.einsum('snc,dnc->nsd', left_side.astype(jnp.float32).reshape(length, N_TP, width), weight.astype(jnp.float32).reshape(weight.shape[0], N_TP, width))
        total = term if total is None else total + term
    return lax.optimization_barrier(jnp.sum(rounded(total), axis=0))

def section(inputs):
    forward_in, backward_in, incoming, documents, w_query, w_key, w_value, w_out = inputs

    def copy_step(totals, item):
        forward_rows, backward_rows, grad_rows, copy_docs = item
        normed_ahead, unused_inverse = norm_rows(forward_rows)
        probs_ahead, mixed_ahead = attend(project(normed_ahead, w_query), project(normed_ahead, w_key), project(normed_ahead, w_value), allowed(copy_docs[0]))
        attended = group_sum([(mixed_ahead, w_out)])
        outgoing = (forward_rows.astype(jnp.float32) + attended).astype(jnp.bfloat16)
        normed_back, inverse_back = norm_rows(backward_rows)
        queries = project(normed_back, w_query)
        keys = project(normed_back, w_key)
        values = project(normed_back, w_value)
        probs_back, unused_mixed = attend(queries, keys, values, allowed(copy_docs[1]))
        dmixed = jnp.dot(grad_rows, w_out, preferred_element_type=jnp.float32).astype(jnp.bfloat16)
        dqueries, dkeys, dvalues = attend_back(dmixed, queries, keys, values, probs_back)
        dkeys = dkeys.astype(jnp.bfloat16)
        dvalues = dvalues.astype(jnp.bfloat16)
        dnormed = group_sum([(dqueries, w_query), (dkeys, w_key), (dvalues, w_value)])
        scaled = backward_rows.astype(jnp.float32) * inverse_back
        grad_back = grad_rows.astype(jnp.float32) + inverse_back * (dnormed - scaled * lax.optimization_barrier(jnp.mean(dnormed * scaled, axis=-1, keepdims=True)))
        new_totals = (totals[0] + rounded(contract_first(normed_back, dqueries)), totals[1] + rounded(contract_first(normed_back, dkeys)), totals[2] + rounded(contract_first(normed_back, dvalues)))
        return (new_totals, (outgoing, grad_back.astype(jnp.bfloat16)))
    zeros = (jnp.zeros((D, HEADS * HEAD), jnp.float32), jnp.zeros((D, KV * SPREAD * HEAD), jnp.float32), jnp.zeros((D, KV * SPREAD * HEAD), jnp.float32))
    totals, (outgoing, grad_back) = lax.scan(copy_step, zeros, (forward_in, backward_in, incoming, documents))
    return (outgoing, grad_back, totals[0], totals[1], totals[2])

def reference(act_in, stash_in, grad_in, doc_ids, query_weight, key_weight, value_weight, out_weight):
    outgoing, grad_back, grad_query, grad_key, grad_value = lax.map(section, (act_in, stash_in, grad_in, doc_ids, query_weight, key_weight, value_weight, out_weight))
    act_out = jnp.roll(outgoing, 1, axis=0)
    grad_out = jnp.roll(grad_back, -1, axis=0)
    return (act_out, grad_out, grad_query, grad_key, grad_value)
```

```python
import functools
import math

import jax
import jax.numpy as jnp
from jax import lax
from jax.experimental import pallas as pl
from jax.experimental.pallas import tpu as pltpu
from jax.sharding import PartitionSpec as P

HEAD = 128


epsilon = 1e-05


def from_behind(value, axis, steps):
    count = lax.axis_size(axis)
    pairs = [(source, (source + steps) % count) for source in range(count)]
    return lax.ppermute(value, axis, pairs)


MESH = pl.DeviceIdType.MESH
VMEM_LIMIT = 60 * 1024 * 1024


def remote(source, target, send_sem, recv_sem, axis, device):
    return pltpu.make_async_remote_copy(
        src_ref=source,
        dst_ref=target,
        send_sem=send_sem,
        recv_sem=recv_sem,
        device_id={axis: device},
        device_id_type=MESH,
    )


def greet(n, copies, me, mine):
    barrier = pltpu.get_barrier_semaphore()

    @pl.when(me > 0)
    def _():
        pl.semaphore_signal(barrier, inc=1, device_id={"tp": me - 1}, device_id_type=MESH)

    @pl.when(me < n - 1)
    def _():
        pl.semaphore_signal(barrier, inc=1, device_id={"tp": me + 1}, device_id_type=MESH)

    for offset in range(1, copies):
        other = lax.rem(mine + offset, copies)
        pl.semaphore_signal(barrier, inc=1, device_id={"dp": other}, device_id_type=MESH)

    ends = jnp.where(me > 0, 1, 0) + jnp.where(me < n - 1, 1, 0)
    pl.semaphore_wait(barrier, ends + copies - 1)


def gather_kernel(
    n, copies,
    act, stash, grad, wq, wk, wv, wo,
    qb, kb, vb, qf, kf, vf, dm, ncols,
    full, normed, vq, vk, vv, vo, wsem, ss, rs, dss, drs,
):
    me = lax.axis_index("tp")
    mine = lax.axis_index("dp")
    rows, width = act.shape
    piece = width // copies
    loads = []
    for i, (hbm, vmem) in enumerate(((wq, vq), (wk, vk), (wv, vv), (wo, vo))):
        load = pltpu.make_async_copy(hbm, vmem, wsem.at[i])
        load.start()
        loads.append(load)
    greet(n, copies, me, mine)
    own = (act, stash, grad)

    def block(a, index):
        return full.at[a, pl.ds(pl.multiple_of(index * rows, rows), rows), :]

    def hop(a, side, step):
        toward = 1 if side == 0 else -1
        carried = me - toward * (step - 1)
        source = own[a] if step == 1 else block(a, carried)
        return remote(
            source, block(a, carried),
            ss.at[a, side, step - 1], rs.at[a, side, step - 1], "tp", me + toward,
        )

    def sends(side, step):
        if side == 0:
            return (me < n - 1) & (me - (step - 1) >= 0)
        return (me > 0) & (me + (step - 1) < n)

    def gets(side, step):
        return (me - step >= 0) if side == 0 else (me + step < n)

    def start(a, step):
        for side in range(2):
            @pl.when(sends(side, step))
            def _():
                hop(a, side, step).start()

    def arrive(a, step):
        for side in range(2):
            @pl.when(gets(side, step))
            def _():
                toward = 1 if side == 0 else -1
                landed = block(a, me - toward * step)
                remote(
                    landed, landed,
                    ss.at[a, side, step - 1], rs.at[a, side, step - 1], "tp",
                    jnp.where(me == 0, 1, me - 1),
                ).wait_recv()

            if step < n - 1:
                @pl.when(sends(side, step + 1))
                def _():
                    hop(a, side, step + 1).start()

    def place(a):
        full[a, pl.ds(pl.multiple_of(me * rows, rows), rows), :] = own[a][...]

    def multiply(left, right, out):
        tile = 256

        @pl.loop(0, right.shape[1] // tile)
        def _(t):
            columns = pl.ds(pl.multiple_of(t * tile, tile), tile)
            out[:, columns] = jnp.dot(
                left[...], right[:, columns], preferred_element_type=jnp.float32
            ).astype(jnp.bfloat16)

    def normalise(a):
        band = 16

        @pl.loop(0, full.shape[1] // band)
        def _(t):
            where = pl.ds(pl.multiple_of(t * band, band), band)
            wide = full[a, where, :].astype(jnp.float32)
            inverse = lax.rsqrt(jnp.mean(wide * wide, axis=-1, keepdims=True) + epsilon)
            normed[where, :] = (wide * inverse).astype(jnp.bfloat16)

    start(0, 1)
    start(1, 1)
    for a in range(3):
        place(a)
    for step in range(1, n):
        arrive(0, step)
    start(2, 1)
    arrive(1, 1)
    normalise(0)
    for load in loads:
        load.wait()
    multiply(normed, vq, qb)
    multiply(normed, vk, kb)
    multiply(normed, vv, vb)
    trades = []
    for offset in range(1, copies):
        other = lax.rem(mine + offset, copies)
        trade = remote(
            normed.at[:, pl.ds(pl.multiple_of(other * piece, piece), piece)],
            ncols.at[mine], dss.at[offset], drs.at[offset], "dp", other,
        )
        trade.start()
        trades.append(trade)
    ncols[mine] = normed[:, pl.ds(pl.multiple_of(mine * piece, piece), piece)]
    for step in range(2, n):
        arrive(1, step)
    arrive(2, 1)
    multiply(full.at[1], vo, dm)
    for step in range(2, n):
        arrive(2, step)
    for trade in trades:
        trade.wait()
    normalise(2)
    multiply(normed, vq, qf)
    multiply(normed, vk, kf)
    multiply(normed, vv, vf)
    for a in range(3):
        for step in range(1, n):
            for side in range(2):
                @pl.when(sends(side, step))
                def _():
                    hop(a, side, step).wait_send()


def gather_call(n, copies, act, grad, stash, wq, wk, wv, wo):
    rows, width = act.shape
    seq = rows * n
    bf = jnp.bfloat16
    vmem = pl.BlockSpec(memory_space=pltpu.VMEM)
    anywhere = pl.BlockSpec(memory_space=pl.ANY)
    shapes = [(seq, w.shape[1]) for w in (wq, wk, wv)] * 2 + [(seq, wo.shape[1])]
    shapes += [(copies, seq, width // copies)]
    sem = pltpu.SemaphoreType.DMA
    return pl.pallas_call(
        functools.partial(gather_kernel, n, copies),
        out_shape=[jax.ShapeDtypeStruct(shape, bf) for shape in shapes],
        in_specs=[vmem] * 3 + [anywhere] * 4,
        out_specs=[vmem] * len(shapes),
        scratch_shapes=[pltpu.VMEM((3, seq, width), bf), pltpu.VMEM((seq, width), bf)]
        + [pltpu.VMEM(w.shape, bf) for w in (wq, wk, wv, wo)]
        + [sem((4,)), sem((3, 2, n)), sem((3, 2, n)), sem((copies,)), sem((copies,))],
        compiler_params=pltpu.CompilerParams(
            collective_id=0, has_side_effects=True, vmem_limit_bytes=VMEM_LIMIT
        ),
        cost_estimate=pl.CostEstimate(
            flops=40_000_000_000, bytes_accessed=30_000_000, transcendentals=0
        ),
    )(stash, grad, act, wq, wk, wv, wo)


def scatter_kernel(
    n, copies,
    fsum, bsum, dq, dk, dv,
    fshare, bshare, aq, ak, av,
    slots, ss, rs, dss, drs,
):
    me = lax.axis_index("tp")
    mine = lax.axis_index("dp")
    rows, width = fshare.shape
    sums = (bsum, fsum)
    greet(n, copies, me, mine)
    trades = []
    for offset in range(1, copies):
        other = lax.rem(mine + offset, copies)
        for i, (source, target) in enumerate(((dq, aq), (dk, ak), (dv, av))):
            trade = remote(
                source, target.at[mine], dss.at[offset, i], drs.at[offset, i], "dp", other
            )
            trade.start()
            trades.append(trade)

    def copy(a, side, dest, first):
        toward = 1 if side == 0 else -1
        part = sums[a].at[pl.ds(dest * rows, rows), :]
        return remote(
            part if first else slots.at[a, side, dest], slots.at[a, side, dest],
            ss.at[a, side, dest], rs.at[a, side, dest], "tp", me + toward,
        )

    def landed(a, side, dest):
        slot = slots.at[a, side, dest]
        remote(
            slot, slot, ss.at[a, side, dest], rs.at[a, side, dest], "tp",
            jnp.where(me == 0, 1, me - 1),
        ).wait_recv()

    def roles(side, dest):
        if side == 0:
            return me == 0, (me > 0) & (me < dest)
        return me == n - 1, (me < n - 1) & (me > dest)

    routes = []
    for k in range(n - 1):
        for side in range(2):
            routes.append((side, n - 1 - k if side == 0 else k))
    for a in range(2):
        for side, dest in routes:
            first, middle = roles(side, dest)

            @pl.when(first)
            def _():
                copy(a, side, dest, True).start()

    aq[mine] = dq[...]
    ak[mine] = dk[...]
    av[mine] = dv[...]
    for a in range(2):
        for side, dest in routes:
            first, middle = roles(side, dest)

            @pl.when(middle)
            def _():
                landed(a, side, dest)
                slots[a, side, dest] = (
                    slots[a, side, dest].astype(jnp.float32)
                    + sums[a][dest * rows : (dest + 1) * rows, :].astype(jnp.float32)
                ).astype(jnp.bfloat16)
                copy(a, side, dest, False).start()

    for a, out in enumerate((bshare, fshare)):
        out[...] = sums[a][pl.ds(pl.multiple_of(me * rows, rows), rows), :].astype(jnp.float32)
        for side, dest in routes:
            @pl.when(me == dest)
            def _():
                landed(a, side, dest)
                out[...] += slots[a, side, dest].astype(jnp.float32)

    for a in range(2):
        for side, dest in routes:
            first, middle = roles(side, dest)

            @pl.when(first | middle)
            def _():
                copy(a, side, dest, False).wait_send()

    for trade in trades:
        trade.wait()


def scatter_call(n, copies, fsum, bsum, dq, dk, dv):
    seq, width = fsum.shape
    rows = seq // n
    vmem = pl.BlockSpec(memory_space=pltpu.VMEM)
    sem = pltpu.SemaphoreType.DMA
    return pl.pallas_call(
        functools.partial(scatter_kernel, n, copies),
        out_shape=[jax.ShapeDtypeStruct((rows, width), jnp.float32)] * 2
        + [jax.ShapeDtypeStruct((copies,) + g.shape, jnp.bfloat16) for g in (dq, dk, dv)],
        in_specs=[vmem] * 5,
        out_specs=[vmem] * 5,
        scratch_shapes=[
            pltpu.VMEM((2, 2, n, rows, width), jnp.bfloat16),
            sem((2, 2, n)), sem((2, 2, n)), sem((copies, 3)), sem((copies, 3)),
        ],
        compiler_params=pltpu.CompilerParams(
            collective_id=1, has_side_effects=True, vmem_limit_bytes=40 * 1024 * 1024
        ),
        cost_estimate=pl.CostEstimate(
            flops=30_000_000_000, bytes_accessed=10_000_000, transcendentals=0
        ),
    )(fsum, bsum, dq, dk, dv)


def weights_kernel(copies, ncols, aq, ak, av, gq, gk, gv):
    for right, out in ((aq, gq), (ak, gk), (av, gv)):
        total = None
        for i in range(copies):
            term = lax.dot_general(
                ncols[i], right[i], (((0,), (0,)), ((), ())),
                preferred_element_type=jnp.float32,
            ).astype(jnp.bfloat16).astype(jnp.float32)
            total = term if total is None else total + term
        out[...] = total


def weights_call(ncols, aq, ak, av):
    copies, seq, piece = ncols.shape
    tile = min(256, piece)
    whole = [
        pl.BlockSpec(g.shape, lambda t: (0, 0, 0)) for g in (aq, ak, av)
    ]
    outs = [jax.ShapeDtypeStruct((piece, g.shape[2]), jnp.float32) for g in (aq, ak, av)]
    return pl.pallas_call(
        functools.partial(weights_kernel, copies),
        grid=(piece // tile,),
        out_shape=outs,
        in_specs=[pl.BlockSpec((copies, seq, tile), lambda t: (0, 0, t))] + whole,
        out_specs=[pl.BlockSpec((tile, o.shape[1]), lambda t: (t, 0)) for o in outs],
        compiler_params=pltpu.CompilerParams(vmem_limit_bytes=40 * 1024 * 1024),
        cost_estimate=pl.CostEstimate(
            flops=2 * copies * seq * piece * sum(o.shape[1] for o in outs),
            bytes_accessed=4 * piece * sum(o.shape[1] for o in outs),
            transcendentals=0,
        ),
    )(ncols, aq, ak, av)


def norm_rows(token_rows):
    widened = token_rows.astype(jnp.float32)
    inverse = lax.rsqrt(jnp.mean(widened * widened, axis=-1, keepdims=True) + epsilon)
    return ((widened * inverse).astype(jnp.bfloat16), inverse)


def allowed(documents):
    length = documents.shape[0]
    position = jnp.arange(length, dtype=jnp.int32)
    return (position[None, :] <= position[:, None]) & (documents[:, None] == documents[None, :])


def contract_last(left_side, right_side):
    return lax.dot_general(
        left_side, right_side, (((1,), (1,)), ((), ())), preferred_element_type=jnp.float32
    )


def split_heads(queries, keys, values, kv_local):
    length = queries.shape[0]
    group_size = queries.shape[1] // (kv_local * HEAD)
    return (
        queries.reshape(length, kv_local, group_size, HEAD),
        keys.reshape(length, kv_local, HEAD),
        values.reshape(length, kv_local, HEAD),
    )


def attend_probs(query_heads, key_heads, allowed_pairs):
    scores = jnp.einsum(
        "ihgd,jhd->hgij", query_heads, key_heads, preferred_element_type=jnp.float32
    ) * (1.0 / math.sqrt(HEAD))
    scores = jnp.where(allowed_pairs, scores, -jnp.inf)
    row_max = jnp.max(scores, axis=-1, keepdims=True)
    weights = jnp.exp(scores - row_max)
    return (weights / jnp.sum(weights, axis=-1, keepdims=True)).astype(jnp.bfloat16)


def attend_back(dmixed, queries, keys, values, probs, kv_local):
    length = queries.shape[0]
    query_heads, key_heads, value_heads = split_heads(queries, keys, values, kv_local)
    dmixed_heads = dmixed.reshape(query_heads.shape)
    dprobs = jnp.einsum(
        "ihgd,jhd->hgij", dmixed_heads, value_heads, preferred_element_type=jnp.float32
    )
    weights = probs.astype(jnp.float32)
    inner = jnp.sum(weights * dprobs, axis=-1, keepdims=True)
    dscores = (weights * (dprobs - inner) * (1.0 / math.sqrt(HEAD))).astype(jnp.bfloat16)
    dqueries = jnp.einsum("hgij,jhd->ihgd", dscores, key_heads, preferred_element_type=jnp.float32)
    dkeys = jnp.einsum("hgij,ihgd->jhd", dscores, query_heads, preferred_element_type=jnp.float32)
    dvalues = jnp.einsum("hgij,ihgd->jhd", probs, dmixed_heads, preferred_element_type=jnp.float32)
    return (
        dqueries.astype(jnp.bfloat16).reshape(length, queries.shape[1]),
        dkeys.reshape(length, kv_local * HEAD),
        dvalues.reshape(length, kv_local * HEAD),
    )


def handoff(payload, offset):
    return from_behind(payload, "pp", offset)


def body(act_in, stash_in, grad_in, doc_ids, query_weight, key_weight, value_weight, out_weight):
    kv_local = key_weight.shape[2] // HEAD
    forward_rows = act_in[0, 0]
    backward_rows = stash_in[0, 0]
    grad_rows = grad_in[0, 0]
    w_query = query_weight[0]
    w_key = key_weight[0]
    w_value = value_weight[0]
    w_out = out_weight[0]
    n, copies = lax.axis_size("tp"), lax.axis_size("dp")
    (
        queries_back, keys_back, values_back, queries_ahead, keys_ahead, values_ahead,
        dmixed, normed_cols,
    ) = gather_call(
        n, copies, forward_rows, grad_rows, backward_rows, w_query, w_key, w_value, w_out
    )
    unused_normed, inverse_back = norm_rows(backward_rows)
    query_heads, key_heads, value_heads = split_heads(
        queries_ahead, keys_ahead, values_ahead, kv_local
    )
    probs_ahead = attend_probs(query_heads, key_heads, allowed(doc_ids[0, 0, 0]))
    mixed_ahead = jnp.einsum(
        "hgij,jhd->ihgd", probs_ahead, value_heads, preferred_element_type=jnp.float32
    )
    mixed_ahead = mixed_ahead.astype(jnp.bfloat16).reshape(queries_ahead.shape)
    forward_sum = contract_last(mixed_ahead, w_out)
    query_back_heads, key_back_heads, unused_values = split_heads(
        queries_back, keys_back, values_back, kv_local
    )
    probs_back = attend_probs(query_back_heads, key_back_heads, allowed(doc_ids[0, 0, 1]))
    dqueries, dkeys, dvalues = attend_back(
        dmixed, queries_back, keys_back, values_back, probs_back, kv_local
    )
    dkey_cols = dkeys.astype(jnp.bfloat16)
    dvalue_cols = dvalues.astype(jnp.bfloat16)
    dnormed = (
        contract_last(dqueries, w_query)
        + contract_last(dkey_cols, w_key)
        + contract_last(dvalue_cols, w_value)
    )
    forward_share, backward_share, all_queries, all_keys, all_values = scatter_call(
        n, copies, forward_sum.astype(jnp.bfloat16), dnormed.astype(jnp.bfloat16),
        dqueries, dkey_cols, dvalue_cols,
    )
    outgoing = (forward_rows.astype(jnp.float32) + forward_share).astype(jnp.bfloat16)
    scaled = backward_rows.astype(jnp.float32) * inverse_back
    grad_back = (
        grad_rows.astype(jnp.float32)
        + inverse_back
        * (backward_share - scaled * jnp.mean(backward_share * scaled, axis=-1, keepdims=True))
    ).astype(jnp.bfloat16)
    act_out = handoff(outgoing, 1)[None, None]
    grad_out = handoff(grad_back, -1)[None, None]
    grad_query, grad_key, grad_value = (
        grad[None] for grad in weights_call(normed_cols, all_queries, all_keys, all_values)
    )
    return (act_out, grad_out, grad_query, grad_key, grad_value)


def solution(mesh):
    placed = (
        P("pp", "dp", "tp", None),
        P("pp", "dp", "tp", None),
        P("pp", "dp", "tp", None),
        P("pp", "dp", None, None),
        P("pp", None, "tp"),
        P("pp", None, "tp"),
        P("pp", None, "tp"),
        P("pp", None, "tp"),
    )
    return jax.shard_map(
        body,
        mesh=mesh,
        in_specs=placed,
        out_specs=(
            P("pp", "dp", "tp", None),
            P("pp", "dp", "tp", None),
            P("pp", "dp", "tp"),
            P("pp", "dp", "tp"),
            P("pp", "dp", "tp"),
        ),
        check_vma=False,
    )
```

```python
import functools
import math

import jax
import jax.numpy as jnp
from jax import lax
from jax.experimental import pallas as pl
from jax.experimental.pallas import tpu as pltpu
from jax.sharding import PartitionSpec as P

HEAD = 128


epsilon = 1e-05


def from_behind(value, axis, steps):
    count = lax.axis_size(axis)
    pairs = [(source, (source + steps) % count) for source in range(count)]
    return lax.ppermute(value, axis, pairs)


MESH = pl.DeviceIdType.MESH
VMEM_LIMIT = 60 * 1024 * 1024


def remote(source, target, send_sem, recv_sem, axis, device):
    return pltpu.make_async_remote_copy(
        src_ref=source,
        dst_ref=target,
        send_sem=send_sem,
        recv_sem=recv_sem,
        device_id={axis: device},
        device_id_type=MESH,
    )


def greet(n, copies, me, mine):
    barrier = pltpu.get_barrier_semaphore()

    @pl.when(me > 0)
    def _():
        pl.semaphore_signal(barrier, inc=1, device_id={"tp": me - 1}, device_id_type=MESH)

    @pl.when(me < n - 1)
    def _():
        pl.semaphore_signal(barrier, inc=1, device_id={"tp": me + 1}, device_id_type=MESH)

    for offset in range(1, copies):
        other = lax.rem(mine + offset, copies)
        pl.semaphore_signal(barrier, inc=1, device_id={"dp": other}, device_id_type=MESH)

    ends = jnp.where(me > 0, 1, 0) + jnp.where(me < n - 1, 1, 0)
    pl.semaphore_wait(barrier, ends + copies - 1)


class LineSum:
    def __init__(self, n, me, rows, whole, slots, ss, rs):
        self.n, self.me, self.rows, self.whole = n, me, rows, whole
        self.slots, self.ss, self.rs = slots, ss, rs

    def routes(self, k):
        return ((0, self.n - 1 - k), (1, k))

    def every(self):
        return [route for k in range(self.n - 1) for route in self.routes(k)]

    def copy(self, side, dest, first):
        part = self.whole.at[pl.ds(dest * self.rows, self.rows), :]
        slot = self.slots.at[side, dest]
        return remote(
            part if first else slot, slot, self.ss.at[side, dest], self.rs.at[side, dest],
            "tp", self.me + (1 if side == 0 else -1),
        )

    def landed(self, side, dest):
        slot = self.slots.at[side, dest]
        remote(
            slot, slot, self.ss.at[side, dest], self.rs.at[side, dest], "tp",
            jnp.where(self.me == 0, 1, self.me - 1),
        ).wait_recv()

    def roles(self, side, dest):
        me, n = self.me, self.n
        if side == 0:
            return me == 0, (me > 0) & (me < dest)
        return me == n - 1, (me < n - 1) & (me > dest)

    def begin(self):
        for side, dest in self.every():
            @pl.when(self.roles(side, dest)[0])
            def _():
                self.copy(side, dest, True).start()

    def middle(self, k):
        slots, rows = self.slots, self.rows
        for side, dest in self.routes(k):
            @pl.when(self.roles(side, dest)[1])
            def _():
                self.landed(side, dest)
                slots[side, dest] = (
                    slots[side, dest].astype(jnp.float32)
                    + self.whole[dest * rows : (dest + 1) * rows, :].astype(jnp.float32)
                ).astype(jnp.bfloat16)
                self.copy(side, dest, False).start()

    def finish(self, out):
        me, rows = self.me, self.rows
        out[...] = self.whole[pl.ds(pl.multiple_of(me * rows, rows), rows), :].astype(jnp.float32)
        for side, dest in self.every():
            @pl.when(me == dest)
            def _():
                self.landed(side, dest)
                out[...] += self.slots[side, dest].astype(jnp.float32)
        for side, dest in self.every():
            first, middle = self.roles(side, dest)

            @pl.when(first | middle)
            def _():
                self.copy(side, dest, False).wait_send()


def gather_kernel(
    n, copies,
    act, stash, grad, mask, wq, wk, wv, wo,
    qb, kb, vb, dm, ncols, fshare,
    full, normed, vq, vk, vv, vo, qf, kf, vf, mixed, fsum, slots,
    wsem, ss, rs, dss, drs, rss, rrs,
):
    me = lax.axis_index("tp")
    mine = lax.axis_index("dp")
    rows, width = act.shape
    piece = width // copies
    loads = []
    for i, (hbm, vmem) in enumerate(((wq, vq), (wk, vk), (wv, vv), (wo, vo))):
        load = pltpu.make_async_copy(hbm, vmem, wsem.at[i])
        load.start()
        loads.append(load)
    greet(n, copies, me, mine)
    own = (act, stash, grad)

    def block(a, index):
        return full.at[a, pl.ds(pl.multiple_of(index * rows, rows), rows), :]

    def hop(a, side, step):
        toward = 1 if side == 0 else -1
        carried = me - toward * (step - 1)
        source = own[a] if step == 1 else block(a, carried)
        return remote(
            source, block(a, carried),
            ss.at[a, side, step - 1], rs.at[a, side, step - 1], "tp", me + toward,
        )

    def sends(side, step):
        if side == 0:
            return (me < n - 1) & (me - (step - 1) >= 0)
        return (me > 0) & (me + (step - 1) < n)

    def gets(side, step):
        return (me - step >= 0) if side == 0 else (me + step < n)

    def start(a, step):
        for side in range(2):
            @pl.when(sends(side, step))
            def _():
                hop(a, side, step).start()

    def arrive(a, step):
        for side in range(2):
            @pl.when(gets(side, step))
            def _():
                toward = 1 if side == 0 else -1
                landed = block(a, me - toward * step)
                remote(
                    landed, landed,
                    ss.at[a, side, step - 1], rs.at[a, side, step - 1], "tp",
                    jnp.where(me == 0, 1, me - 1),
                ).wait_recv()

            if step < n - 1:
                @pl.when(sends(side, step + 1))
                def _():
                    hop(a, side, step + 1).start()

    def place(a):
        full[a, pl.ds(pl.multiple_of(me * rows, rows), rows), :] = own[a][...]

    def multiply(left, right, out):
        tile = 256

        @pl.loop(0, right.shape[1] // tile)
        def _(t):
            columns = pl.ds(pl.multiple_of(t * tile, tile), tile)
            out[:, columns] = jnp.dot(
                left[...], right[:, columns], preferred_element_type=jnp.float32
            ).astype(jnp.bfloat16)

    def normalise(a):
        band = 16

        @pl.loop(0, full.shape[1] // band)
        def _(t):
            where = pl.ds(pl.multiple_of(t * band, band), band)
            wide = full[a, where, :].astype(jnp.float32)
            inverse = lax.rsqrt(jnp.mean(wide * wide, axis=-1, keepdims=True) + epsilon)
            normed[where, :] = (wide * inverse).astype(jnp.bfloat16)

    def attend():
        heads = qf.shape[1] // HEAD
        group_size = qf.shape[1] // kf.shape[1]
        for h in range(heads):
            columns = slice(h * HEAD, (h + 1) * HEAD)
            k = h // group_size
            kv_columns = slice(k * HEAD, (k + 1) * HEAD)
            scores = contract_last(qf[:, columns], kf[:, kv_columns]) * (1.0 / math.sqrt(HEAD))
            scores = jnp.where(mask[...] > 0.5, scores, -jnp.inf)
            weights = jnp.exp(scores - jnp.max(scores, axis=-1, keepdims=True))
            probs = (weights / jnp.sum(weights, axis=-1, keepdims=True)).astype(jnp.bfloat16)
            mixed[:, columns] = jnp.dot(
                probs, vf[:, kv_columns], preferred_element_type=jnp.float32
            ).astype(jnp.bfloat16)

    def project_out():
        tile = 256

        @pl.loop(0, width // tile)
        def _(t):
            features = pl.ds(pl.multiple_of(t * tile, tile), tile)
            fsum[:, features] = contract_last(mixed[...], vo[features, :]).astype(jnp.bfloat16)

    line = LineSum(n, me, rows, fsum, slots, rss, rrs)
    start(0, 1)
    start(1, 1)
    for a in range(3):
        place(a)
    for step in range(1, n):
        arrive(0, step)
    start(2, 1)
    arrive(1, 1)
    normalise(0)
    for load in loads:
        load.wait()
    multiply(normed, vq, qf)
    multiply(normed, vk, kf)
    multiply(normed, vv, vf)
    for step in range(2, n):
        arrive(1, step)
    attend()
    arrive(2, 1)
    project_out()
    line.begin()
    normalise(1)
    multiply(normed, vq, qb)
    trades = []
    for offset in range(1, copies):
        other = lax.rem(mine + offset, copies)
        trade = remote(
            normed.at[:, pl.ds(pl.multiple_of(other * piece, piece), piece)],
            ncols.at[mine], dss.at[offset], drs.at[offset], "dp", other,
        )
        trade.start()
        trades.append(trade)
    ncols[mine] = normed[:, pl.ds(pl.multiple_of(mine * piece, piece), piece)]
    arrive(2, 2) if n > 2 else None
    line.middle(0)
    multiply(normed, vk, kb)
    multiply(normed, vv, vb)
    for step in range(3, n):
        arrive(2, step)
        line.middle(step - 2)
    if n > 2:
        line.middle(n - 2)
    multiply(full.at[2], vo, dm)
    line.finish(fshare)
    for trade in trades:
        trade.wait()
    for a in range(3):
        for step in range(1, n):
            for side in range(2):
                @pl.when(sends(side, step))
                def _():
                    hop(a, side, step).wait_send()


def gather_call(n, copies, act, grad, stash, mask, wq, wk, wv, wo):
    rows, width = act.shape
    seq = rows * n
    bf = jnp.bfloat16
    vmem = pl.BlockSpec(memory_space=pltpu.VMEM)
    anywhere = pl.BlockSpec(memory_space=pl.ANY)
    heads = [(seq, w.shape[1]) for w in (wq, wk, wv)]
    shapes = heads + [(seq, wo.shape[1])]
    shapes += [(copies, seq, width // copies)]
    sem = pltpu.SemaphoreType.DMA
    return pl.pallas_call(
        functools.partial(gather_kernel, n, copies),
        out_shape=[jax.ShapeDtypeStruct(shape, bf) for shape in shapes]
        + [jax.ShapeDtypeStruct((rows, width), jnp.float32)],
        in_specs=[vmem] * 4 + [anywhere] * 4,
        out_specs=[vmem] * (len(shapes) + 1),
        scratch_shapes=[pltpu.VMEM((3, seq, width), bf), pltpu.VMEM((seq, width), bf)]
        + [pltpu.VMEM(w.shape, bf) for w in (wq, wk, wv, wo)]
        + [pltpu.VMEM(shape, bf) for shape in heads]
        + [pltpu.VMEM((seq, wo.shape[1]), bf), pltpu.VMEM((seq, width), bf)]
        + [pltpu.VMEM((2, n, rows, width), bf)]
        + [sem((4,)), sem((3, 2, n)), sem((3, 2, n)), sem((copies,)), sem((copies,))]
        + [sem((2, n)), sem((2, n))],
        compiler_params=pltpu.CompilerParams(
            collective_id=0, has_side_effects=True, vmem_limit_bytes=VMEM_LIMIT
        ),
        cost_estimate=pl.CostEstimate(
            flops=40_000_000_000, bytes_accessed=30_000_000, transcendentals=0
        ),
    )(act, stash, grad, mask, wq, wk, wv, wo)


def scatter_kernel(
    n, copies,
    bsum, dq, dk, dv,
    bshare, aq, ak, av,
    slots, ss, rs, dss, drs,
):
    me = lax.axis_index("tp")
    mine = lax.axis_index("dp")
    rows = bshare.shape[0]
    greet(n, copies, me, mine)
    trades = []
    for offset in range(1, copies):
        other = lax.rem(mine + offset, copies)
        for i, (source, target) in enumerate(((dq, aq), (dk, ak), (dv, av))):
            trade = remote(
                source, target.at[mine], dss.at[offset, i], drs.at[offset, i], "dp", other
            )
            trade.start()
            trades.append(trade)

    line = LineSum(n, me, rows, bsum, slots, ss, rs)
    line.begin()
    aq[mine] = dq[...]
    ak[mine] = dk[...]
    av[mine] = dv[...]
    for k in range(n - 1):
        line.middle(k)
    line.finish(bshare)
    for trade in trades:
        trade.wait()


def scatter_call(n, copies, bsum, dq, dk, dv):
    seq, width = bsum.shape
    rows = seq // n
    vmem = pl.BlockSpec(memory_space=pltpu.VMEM)
    sem = pltpu.SemaphoreType.DMA
    return pl.pallas_call(
        functools.partial(scatter_kernel, n, copies),
        out_shape=[jax.ShapeDtypeStruct((rows, width), jnp.float32)]
        + [jax.ShapeDtypeStruct((copies,) + g.shape, jnp.bfloat16) for g in (dq, dk, dv)],
        in_specs=[vmem] * 4,
        out_specs=[vmem] * 4,
        scratch_shapes=[
            pltpu.VMEM((2, n, rows, width), jnp.bfloat16),
            sem((2, n)), sem((2, n)), sem((copies, 3)), sem((copies, 3)),
        ],
        compiler_params=pltpu.CompilerParams(
            collective_id=1, has_side_effects=True, vmem_limit_bytes=40 * 1024 * 1024
        ),
        cost_estimate=pl.CostEstimate(
            flops=30_000_000_000, bytes_accessed=10_000_000, transcendentals=0
        ),
    )(bsum, dq, dk, dv)


def weights_kernel(copies, ncols, aq, ak, av, gq, gk, gv):
    for right, out in ((aq, gq), (ak, gk), (av, gv)):
        total = None
        for i in range(copies):
            term = lax.dot_general(
                ncols[i], right[i], (((0,), (0,)), ((), ())),
                preferred_element_type=jnp.float32,
            ).astype(jnp.bfloat16).astype(jnp.float32)
            total = term if total is None else total + term
        out[...] = total


def weights_call(ncols, aq, ak, av):
    copies, seq, piece = ncols.shape
    tile = min(256, piece)
    whole = [
        pl.BlockSpec(g.shape, lambda t: (0, 0, 0)) for g in (aq, ak, av)
    ]
    outs = [jax.ShapeDtypeStruct((piece, g.shape[2]), jnp.float32) for g in (aq, ak, av)]
    return pl.pallas_call(
        functools.partial(weights_kernel, copies),
        grid=(piece // tile,),
        out_shape=outs,
        in_specs=[pl.BlockSpec((copies, seq, tile), lambda t: (0, 0, t))] + whole,
        out_specs=[pl.BlockSpec((tile, o.shape[1]), lambda t: (t, 0)) for o in outs],
        compiler_params=pltpu.CompilerParams(vmem_limit_bytes=40 * 1024 * 1024),
        cost_estimate=pl.CostEstimate(
            flops=2 * copies * seq * piece * sum(o.shape[1] for o in outs),
            bytes_accessed=4 * piece * sum(o.shape[1] for o in outs),
            transcendentals=0,
        ),
    )(ncols, aq, ak, av)


def norm_rows(token_rows):
    widened = token_rows.astype(jnp.float32)
    inverse = lax.rsqrt(jnp.mean(widened * widened, axis=-1, keepdims=True) + epsilon)
    return ((widened * inverse).astype(jnp.bfloat16), inverse)


def allowed(documents):
    length = documents.shape[0]
    position = jnp.arange(length, dtype=jnp.int32)
    return (position[None, :] <= position[:, None]) & (documents[:, None] == documents[None, :])


def contract_last(left_side, right_side):
    return lax.dot_general(
        left_side, right_side, (((1,), (1,)), ((), ())), preferred_element_type=jnp.float32
    )


def split_heads(queries, keys, values, kv_local):
    length = queries.shape[0]
    group_size = queries.shape[1] // (kv_local * HEAD)
    return (
        queries.reshape(length, kv_local, group_size, HEAD),
        keys.reshape(length, kv_local, HEAD),
        values.reshape(length, kv_local, HEAD),
    )


def attend_probs(query_heads, key_heads, allowed_pairs):
    scores = jnp.einsum(
        "ihgd,jhd->hgij", query_heads, key_heads, preferred_element_type=jnp.float32
    ) * (1.0 / math.sqrt(HEAD))
    scores = jnp.where(allowed_pairs, scores, -jnp.inf)
    row_max = jnp.max(scores, axis=-1, keepdims=True)
    weights = jnp.exp(scores - row_max)
    return (weights / jnp.sum(weights, axis=-1, keepdims=True)).astype(jnp.bfloat16)


def attend_back(dmixed, queries, keys, values, probs, kv_local):
    length = queries.shape[0]
    query_heads, key_heads, value_heads = split_heads(queries, keys, values, kv_local)
    dmixed_heads = dmixed.reshape(query_heads.shape)
    dprobs = jnp.einsum(
        "ihgd,jhd->hgij", dmixed_heads, value_heads, preferred_element_type=jnp.float32
    )
    weights = probs.astype(jnp.float32)
    inner = jnp.sum(weights * dprobs, axis=-1, keepdims=True)
    dscores = (weights * (dprobs - inner) * (1.0 / math.sqrt(HEAD))).astype(jnp.bfloat16)
    dqueries = jnp.einsum("hgij,jhd->ihgd", dscores, key_heads, preferred_element_type=jnp.float32)
    dkeys = jnp.einsum("hgij,ihgd->jhd", dscores, query_heads, preferred_element_type=jnp.float32)
    dvalues = jnp.einsum("hgij,ihgd->jhd", probs, dmixed_heads, preferred_element_type=jnp.float32)
    return (
        dqueries.astype(jnp.bfloat16).reshape(length, queries.shape[1]),
        dkeys.reshape(length, kv_local * HEAD),
        dvalues.reshape(length, kv_local * HEAD),
    )


def handoff(payload, offset):
    return from_behind(payload, "pp", offset)


def body(act_in, stash_in, grad_in, doc_ids, query_weight, key_weight, value_weight, out_weight):
    kv_local = key_weight.shape[2] // HEAD
    forward_rows = act_in[0, 0]
    backward_rows = stash_in[0, 0]
    grad_rows = grad_in[0, 0]
    w_query = query_weight[0]
    w_key = key_weight[0]
    w_value = value_weight[0]
    w_out = out_weight[0]
    n, copies = lax.axis_size("tp"), lax.axis_size("dp")
    queries_back, keys_back, values_back, dmixed, normed_cols, forward_share = gather_call(
        n, copies, forward_rows, grad_rows, backward_rows,
        allowed(doc_ids[0, 0, 0]).astype(jnp.float32), w_query, w_key, w_value, w_out,
    )
    unused_normed, inverse_back = norm_rows(backward_rows)
    query_back_heads, key_back_heads, unused_values = split_heads(
        queries_back, keys_back, values_back, kv_local
    )
    probs_back = attend_probs(query_back_heads, key_back_heads, allowed(doc_ids[0, 0, 1]))
    dqueries, dkeys, dvalues = attend_back(
        dmixed, queries_back, keys_back, values_back, probs_back, kv_local
    )
    dkey_cols = dkeys.astype(jnp.bfloat16)
    dvalue_cols = dvalues.astype(jnp.bfloat16)
    dnormed = (
        contract_last(dqueries, w_query)
        + contract_last(dkey_cols, w_key)
        + contract_last(dvalue_cols, w_value)
    )
    backward_share, all_queries, all_keys, all_values = scatter_call(
        n, copies, dnormed.astype(jnp.bfloat16), dqueries, dkey_cols, dvalue_cols
    )
    outgoing = (forward_rows.astype(jnp.float32) + forward_share).astype(jnp.bfloat16)
    scaled = backward_rows.astype(jnp.float32) * inverse_back
    grad_back = (
        grad_rows.astype(jnp.float32)
        + inverse_back
        * (backward_share - scaled * jnp.mean(backward_share * scaled, axis=-1, keepdims=True))
    ).astype(jnp.bfloat16)
    act_out = handoff(outgoing, 1)[None, None]
    grad_out = handoff(grad_back, -1)[None, None]
    grad_query, grad_key, grad_value = (
        grad[None] for grad in weights_call(normed_cols, all_queries, all_keys, all_values)
    )
    return (act_out, grad_out, grad_query, grad_key, grad_value)


def solution(mesh):
    placed = (
        P("pp", "dp", "tp", None),
        P("pp", "dp", "tp", None),
        P("pp", "dp", "tp", None),
        P("pp", "dp", None, None),
        P("pp", None, "tp"),
        P("pp", None, "tp"),
        P("pp", None, "tp"),
        P("pp", None, "tp"),
    )
    return jax.shard_map(
        body,
        mesh=mesh,
        in_specs=placed,
        out_specs=(
            P("pp", "dp", "tp", None),
            P("pp", "dp", "tp", None),
            P("pp", "dp", "tp"),
            P("pp", "dp", "tp"),
            P("pp", "dp", "tp"),
        ),
        check_vma=False,
    )
```
